32 devices in a mesh: tp: 4 (over z), pp: 8 (over y, x, core).
Axes of the slice: x: 2, y: 2, z: 4, core: 2. Of those that a mesh axis runs over, the one named last changes fastest.
Arguments:
- tokens: bfloat16 [8192, 8192], P('pp', 'tp'), may hold values from -60 to 60
- norm_gain: bfloat16 [8192], P('tp'), may hold values from 0.099609375 to 1.8984375
- weights_gen: bfloat16 [8, 1280, 8192], P('tp', None, 'pp'), may hold values from -2 to 2
- segment_ids: int32 [8, 1024], P('pp'), may hold values from 0 to 15, never falling along the last dimension, each value on 1 to 512 neighbouring positions
Outputs:
- weights_rows: bfloat16 [8, 1280, 8192], P('tp', 'pp')
- attended: bfloat16 [8192, 8192], P('pp', 'tp')
The draws below stay inside these ranges and needn't reach their ends.
Inputs may be any that keep to these rules, and one draw needn't show every extreme that they name: `segment_ids`: ids never fall along a block; every sequence has 1 to 512 tokens and lies in one block.
All inputs are finite; a program needn't handle non-finite values.
Results may differ from the reference program's by a relative error of at most 0.0075.
Values may be sent and summed in bfloat16 or wider, within the bound.
A program may use at most 192 MiB of HBM per device.

```python
import math
import jax
import jax.numpy as jnp
import numpy as np
from jax import lax

D = 8192
HQ = 64
KVH = 8
DH = 128
TOK_DEV = 1024
GROUP = 8
QROWS = 1280
BLOCKS = 8
TOKENS = 8192
SEGS = 16


def draw_tokens(key, part):
    first = jax.random.fold_in(jax.random.fold_in(key, 11), 0)
    base = jax.random.truncated_normal(first, -6.0, 6.0, (TOKENS, D), jnp.float32)
    return jnp.clip(base, -60.0, 60.0).astype(jnp.bfloat16)


def draw_weights_gen(key, part):
    first = jax.random.fold_in(jax.random.fold_in(key, 23), 0)
    base = jax.random.truncated_normal(first, -6.0, 6.0, (KVH, QROWS, D), jnp.float32) / math.sqrt(D)
    return jnp.clip(base, -2.0, 2.0).astype(jnp.bfloat16)


def length_profile(count, total, limit, lean):
    portions = [(1 << 20) // math.isqrt(rank ** lean) + 1 for rank in range(2, count + 1)]
    rest, counts = total - limit - (count - 1), [1] * (count - 1)
    while rest > 0:
        candidates = [i for i in range(count - 1) if counts[i] < limit]
        whole, budget = sum([portions[i] for i in candidates]), rest
        for i in candidates:
            addition = min(limit - counts[i], max(1, budget * portions[i] // whole), rest)
            counts[i] = counts[i] + addition
            rest = rest - addition
    return np.array([limit] + counts)


def uneven_parts(rng, amount, total, limit, lean):
    if amount == 2:
        one = jax.random.randint(rng, (), max(1, total - limit), min(limit, total - 1) + 1)
        return jnp.stack([one, total - one])
    lengths = jnp.asarray(length_profile(amount, total, limit, lean), jnp.int32)
    pairs = (amount - 1) // 2
    donor, taker = lengths[1:1 + 2 * pairs:2], lengths[2:2 + 2 * pairs:2]
    margin = jnp.minimum(donor - 1, limit - taker)
    passed = jax.random.randint(jax.random.fold_in(rng, 1), (pairs,), 0, 1 << 20) % (margin + 1)
    lengths = lengths.at[1:1 + 2 * pairs:2].set(donor - passed).at[2:2 + 2 * pairs:2].set(taker + passed)
    return lengths[jax.random.permutation(jax.random.fold_in(rng, 2), amount)]


def setup_inputs(seed: int = 0) -> dict:
    splits = jax.random.split(jax.random.key(seed), 5)
    return {
        "tokens": draw_tokens(jax.random.fold_in(splits[4], 71), 0),
        "norm_gain": jnp.clip(1.0 + 0.18 * jax.random.normal(splits[1], (D,), jnp.float32), 0.099609375, 1.8984375).astype(jnp.bfloat16),
        "weights_gen": draw_weights_gen(jax.random.fold_in(splits[4], 71), 0),
        "segment_ids": jax.vmap(lambda own: jnp.searchsorted(jnp.cumsum(uneven_parts(own, SEGS, TOK_DEV, TOK_DEV // 2, 1)), jnp.arange(TOK_DEV), side="right"))(jax.random.split(splits[3], BLOCKS)).reshape((BLOCKS, TOK_DEV)).astype(jnp.int32),
    }


rope_base = 500000.0

def rotary(values, positions):
    half = values.shape[-1] // 2
    freq = jnp.exp(jnp.arange(half, dtype=jnp.float32) * (-2.0 * math.log(rope_base) / values.shape[-1]))
    angle = positions.astype(jnp.float32)[:, None] * freq[None, :]
    cosine = jnp.cos(angle)
    sine = jnp.sin(angle)
    extra = values.ndim - 2
    cosine = cosine.reshape(cosine.shape[:1] + (1,) * extra + cosine.shape[1:])
    sine = sine.reshape(sine.shape[:1] + (1,) * extra + sine.shape[1:])
    first = values[..., :half]
    second = values[..., half:]
    return jnp.concatenate([first * cosine - second * sine, second * cosine + first * sine], axis=-1)

def block_positions(seg):
    count = seg.shape[0]
    start = lax.optimization_barrier(jnp.sum((seg[None, :] < seg[:, None]).astype(jnp.int32), axis=1))
    return jnp.arange(count, dtype=jnp.int32) - start

def attend_block(query, key, value, seg):
    count = seg.shape[0]
    score = jnp.einsum('tgjd,sgd->gjts', query.astype(jnp.float32), key.astype(jnp.float32)) * (1.0 / math.sqrt(DH))
    order = jnp.arange(count, dtype=jnp.int32)
    allowed = (seg[:, None] == seg[None, :]) & (order[:, None] >= order[None, :])
    score = jnp.where(allowed[None, None], score, -1e+30)
    top = lax.optimization_barrier(jnp.max(score, axis=-1, keepdims=True))
    expo = jnp.where(allowed[None, None], jnp.exp(score - top), 0.0)
    prob = (expo / lax.optimization_barrier(jnp.sum(expo, axis=-1, keepdims=True))).astype(jnp.bfloat16)
    out = jnp.einsum('gjts,sgd->tgjd', prob.astype(jnp.float32), value.astype(jnp.float32))
    return out.astype(jnp.bfloat16).reshape(count, -1)

def reference(tokens, norm_gain, weights_gen, segment_ids):
    floats = tokens.astype(jnp.float32)
    square = lax.optimization_barrier(jnp.mean(floats * floats, axis=-1, keepdims=True))
    normed = (floats * lax.rsqrt(square + 1e-05) * norm_gain.astype(jnp.float32)).astype(jnp.bfloat16)
    flat = weights_gen.reshape(KVH * QROWS, D)
    mixed = jnp.dot(normed, flat.T, preferred_element_type=jnp.float32)
    mixed = mixed.reshape(TOKENS, KVH, GROUP + 2, DH)
    positions = jax.vmap(block_positions)(segment_ids).reshape(TOKENS)
    query = rotary(mixed[:, :, :GROUP, :], positions).astype(jnp.bfloat16)
    key = rotary(mixed[:, :, GROUP, :], positions).astype(jnp.bfloat16)
    value = mixed[:, :, GROUP + 1, :].astype(jnp.bfloat16)
    query = query.reshape(BLOCKS, TOK_DEV, KVH, GROUP, DH)
    key = key.reshape(BLOCKS, TOK_DEV, KVH, DH)
    value = value.reshape(BLOCKS, TOK_DEV, KVH, DH)

    def one_block(items):
        return attend_block(items[0], items[1], items[2], items[3])
    attended = lax.map(one_block, (query, key, value, segment_ids))
    return (weights_gen, attended.reshape(TOKENS, HQ * DH))
```

```python
import functools
import math

import jax
import jax.numpy as jnp
from jax import lax
from jax.sharding import PartitionSpec as P


DH = 128
GROUP = 8


rope_base = 500000.0


def rotary(values, positions):
    half = values.shape[-1] // 2
    freq = jnp.exp(
        jnp.arange(half, dtype=jnp.float32) * (-2.0 * math.log(rope_base) / values.shape[-1])
    )
    angle = positions.astype(jnp.float32)[:, None] * freq[None, :]
    cosine = jnp.cos(angle)
    sine = jnp.sin(angle)
    extra = values.ndim - 2
    cosine = cosine.reshape(cosine.shape[:1] + (1,) * extra + cosine.shape[1:])
    sine = sine.reshape(sine.shape[:1] + (1,) * extra + sine.shape[1:])
    first = values[..., :half]
    second = values[..., half:]
    return jnp.concatenate(
        [first * cosine - second * sine, second * cosine + first * sine], axis=-1
    )


MAX_SEQUENCE = 512


def layer(size, *arguments):
    return shards(size, *arguments)


def shards(size, tokens, norm_gain, weights_gen, segment_ids):
    pieces = lax.all_gather(weights_gen, "pp", axis=0)
    parts, groups, rows, width = pieces.shape
    kept = rows // parts
    own = lax.dynamic_slice_in_dim(pieces, lax.axis_index("pp") * kept, kept, axis=2)
    weights_rows = own.transpose(1, 2, 0, 3).reshape(groups, kept, parts * width)

    count, local = tokens.shape
    floats = tokens.astype(jnp.float32)
    squares = lax.all_gather(jnp.sum(floats * floats, axis=-1), "tp", axis=0)
    square = jnp.sum(squares, axis=0)[:, None] * (1.0 / (size * local))
    normed = (floats * lax.rsqrt(square + 1e-05) * norm_gain.astype(jnp.float32)).astype(jnp.bfloat16)

    me = lax.axis_index("tp")
    per = local // width

    def added(total, block, owner):
        owner = jnp.clip(owner, 0, size - 1)
        for p in range(per):
            piece = lax.dynamic_index_in_dim(pieces, owner * per + p, axis=0, keepdims=False)
            term = jnp.einsum(
                "td,grd->tgr",
                block[:, p * width : (p + 1) * width],
                piece,
                preferred_element_type=jnp.float32,
            )
            total = lax.optimization_barrier(term if total is None else total + term)
        return total

    up = down = normed
    mixed = added(None, normed, me)
    for step in range(1, size):
        up = lax.ppermute(up, "tp", [(i, i + 1) for i in range(step - 1, size - 1)])
        down = lax.ppermute(down, "tp", [(i + 1, i) for i in range(size - step)])
        if 2 * step >= size:
            below = me >= step
            mixed = added(mixed, jnp.where(below, up, down), jnp.where(below, me - step, me + step))
        else:
            mixed = added(mixed, up, me - step)
            mixed = added(mixed, down, me + step)
    mixed = mixed.reshape(count, groups, GROUP + 2, DH)
    seg = segment_ids[0]
    order = jnp.arange(count, dtype=jnp.int32)
    start_index = jnp.sum((seg[None, :] < seg[:, None]).astype(jnp.int32), axis=1)
    positions = order - start_index
    query = rotary(mixed[:, :, :GROUP, :], positions).astype(jnp.bfloat16)
    key_heads = rotary(mixed[:, :, GROUP, :], positions).astype(jnp.bfloat16)
    value_heads = mixed[:, :, GROUP + 1, :].astype(jnp.bfloat16)
    chunk = count // 4
    outputs = []
    for c in range(4):
        low, high = c * chunk, (c + 1) * chunk
        first = max(0, (low - MAX_SEQUENCE + 1) // chunk * chunk)
        score = jnp.einsum(
            "tgjd,sgd->gjts",
            query[low:high],
            key_heads[first:high],
            preferred_element_type=jnp.float32,
        ) * (1.0 / math.sqrt(DH))
        allowed = (seg[low:high, None] == seg[None, first:high]) & (
            order[low:high, None] >= order[None, first:high]
        )
        score = jnp.where(allowed[None, None], score, -1e30)
        top = jnp.max(score, axis=-1, keepdims=True)
        expo = jnp.where(allowed[None, None], jnp.exp(score - top), 0.0)
        prob = (expo / jnp.sum(expo, axis=-1, keepdims=True)).astype(jnp.bfloat16)
        output = jnp.einsum(
            "gjts,sgd->tgjd", prob, value_heads[first:high], preferred_element_type=jnp.float32
        )
        outputs.append(output.astype(jnp.bfloat16).reshape(chunk, groups * GROUP * DH))
    attended = jnp.concatenate(outputs, axis=0)
    return (weights_rows, attended)


def solution(mesh):
    in_specs = (P("pp", "tp"), P("tp"), P("tp", None, "pp"), P("pp", None))
    out_specs = (P("tp", "pp", None), P("pp", "tp"))
    return jax.shard_map(
        functools.partial(layer, mesh.shape["tp"]),
        mesh=mesh,
        in_specs=in_specs,
        out_specs=out_specs,
        check_vma=False,
    )
```
